32 devices in a mesh: dp: 16 (over z, x, core), tensor: 2 (over y).
Axes of the slice: x: 2, y: 2, z: 4, core: 2. Of those that a mesh axis runs over, the one named last changes fastest.
Arguments:
- drafter_hidden: bfloat16 [2, 2048, 4096], P(None, 'dp', 'tensor'), may hold values from -2000 to 2000
- norm_gain: bfloat16 [4096], P('tensor'), may hold values from 0.5 to 1.5
- head_weight: bfloat16 [4096, 8192], P('tensor', 'dp'), may hold values from -24 to 24
- labels: int32 [2048], P('dp'), may hold values from 0 to 8191
- loss_mask: int32 [2048], P('dp'), may hold values 0 or 1
- offsets: int32 [2], replicated, may hold values from 1 to 4
Outputs:
- draft_loss: float32 [], replicated
- head_grad: float32 [4096, 8192], P('tensor', 'dp')
The draws below stay inside these ranges and needn't reach their ends.
All inputs are finite; a program needn't handle non-finite values. No bound on the sum of `loss_mask` on one device may be relied on, other than what follows from the above.
Results may differ from the reference program's by a relative error of at most 0.0048.
Values may be sent and summed in bfloat16 or wider, within the bound.
A program may use at most 128 MiB of HBM per device.

```python
import math
import jax
import jax.numpy as jnp
from jax import lax

D = 4096
STEPS = 2
WINDOW = 512
MAXOFF = 4
TOKENS = 2048
VOCAB = 8192


def shared_head(key):
    head_key = jax.random.fold_in(key, 11)
    values = jax.random.truncated_normal(head_key, -6.0, 6.0, (D, VOCAB), jnp.float32)
    loud = max(1.0, 48.0 / math.sqrt(D))
    column_ids = jnp.arange(VOCAB)
    boost = jnp.where(column_ids % 8 == 3, loud, 1.0).astype(jnp.float32)
    return values * (5.0 / math.sqrt(D)) * boost[None, :]


def draw_head_weight(key, part):
    return shared_head(key).astype(jnp.bfloat16)


def draw_drafter_hidden(key, part):
    noise_key = jax.random.fold_in(key, 21)
    scale_key = jax.random.fold_in(key, 22)
    first_key = jax.random.fold_in(key, 24)
    second_key = jax.random.fold_in(key, 25)
    noise = jax.random.truncated_normal(noise_key, -6.0, 6.0, (STEPS, TOKENS, D), jnp.float32)
    row_scale = jnp.exp(jax.random.uniform(scale_key, (STEPS, TOKENS, 1), jnp.float32, 0.0, math.log(10.0)))
    head_rows = shared_head(key).T
    groups = VOCAB // 8
    first = 8 * jax.random.randint(first_key, (STEPS, TOKENS), 0, groups) + 3
    second = (first + 8 * jax.random.randint(second_key, (STEPS, TOKENS), 1, groups)) % VOCAB
    positions = jnp.arange(TOKENS)
    chosen = (positions % 61 == 7)[None, :, None]
    strengths = jnp.array([0.5, 1.0, 2.0, 3.0], jnp.float32)[positions // 61 % 4][None, :, None]
    signal = strengths * 8.0 * (head_rows[first] + 0.99 * head_rows[second])
    mixed = jnp.where(chosen, noise + signal, noise)
    return jnp.clip(mixed * row_scale, -2000.0, 2000.0).astype(jnp.bfloat16)


def with_ends(drawn, stream_key, least, top_value):
    place = [jax.random.randint(jax.random.fold_in(stream_key, axis), (), 0, length) for axis, length in enumerate(drawn.shape)]
    widest = drawn.shape.index(max(drawn.shape))
    beside = place[:widest] + [(place[widest] + 1) % drawn.shape[widest]] + place[widest + 1:]
    return drawn.at[tuple(place)].set(least).at[tuple(beside)].set(top_value)


def setup_inputs(seed: int = 0) -> dict:
    streams_of = jax.random.split(jax.random.key(seed), 7)
    drafter_hidden = draw_drafter_hidden(jax.random.fold_in(streams_of[6], 71), 0)
    norm_gain = jnp.clip(1.0 + 0.1 * jax.random.normal(streams_of[1], (D,), jnp.float32), 0.5, 1.5).astype(jnp.bfloat16)
    head_weight = draw_head_weight(jax.random.fold_in(streams_of[6], 71), 0)
    labels = with_ends(jax.random.randint(streams_of[3], (TOKENS,), 0, VOCAB), jax.random.fold_in(streams_of[3], 1), 0, VOCAB - 1).astype(jnp.int32)
    loss_mask = with_ends((jax.random.randint(streams_of[4], (TOKENS,), 0, 4) < 3).astype(jnp.int32), jax.random.fold_in(streams_of[4], 1), 0, 1)
    offsets = jax.random.randint(streams_of[5], (STEPS,), 1, MAXOFF + 1).astype(jnp.int32)
    return dict(drafter_hidden=drafter_hidden, norm_gain=norm_gain, head_weight=head_weight, labels=labels, loss_mask=loss_mask, offsets=offsets)


epsilon = 1e-05
step_decay = 0.8

def reference(drafter_hidden, norm_gain, head_weight, labels, loss_mask, offsets):
    hidden_wide = drafter_hidden.astype(jnp.float32)
    inverse = lax.rsqrt(lax.optimization_barrier(jnp.mean(hidden_wide * hidden_wide, axis=-1, keepdims=True)) + epsilon)
    normed = (hidden_wide * inverse * norm_gain.astype(jnp.float32)).astype(jnp.bfloat16)
    weight_wide = head_weight.astype(jnp.float32)
    positions = jnp.arange(TOKENS, dtype=jnp.int32)
    columns = jnp.arange(VOCAB, dtype=jnp.int32)
    block_rows = min(512, TOKENS)
    gradient = jnp.zeros((D, VOCAB), jnp.float32)
    loss_total = jnp.zeros((), jnp.float32)
    for step_at in range(STEPS):
        factor = step_decay ** step_at
        inside = positions % WINDOW + offsets[step_at] < WINDOW
        clamped = jnp.minimum(positions + offsets[step_at], TOKENS - 1).astype(jnp.int32)
        row_label = labels[clamped]
        row_weight = jnp.where(inside, loss_mask[clamped], 0).astype(jnp.float32)
        counted = jnp.sum(row_weight)
        rows_step = normed[step_at]

        def one_block(state_pair, number):
            offset_row = (number * block_rows).astype(jnp.int32)
            row_block = lax.dynamic_slice_in_dim(rows_step, offset_row, block_rows, 0)
            block_label = lax.dynamic_slice_in_dim(row_label, offset_row, block_rows, 0)
            block_weight = lax.dynamic_slice_in_dim(row_weight, offset_row, block_rows, 0)
            rows_wide = row_block.astype(jnp.float32)
            logits = jnp.dot(rows_wide, weight_wide, precision=lax.Precision.HIGHEST)
            row_top = lax.optimization_barrier(jnp.max(logits, axis=-1))
            total_exp = lax.optimization_barrier(jnp.sum(jnp.exp(logits - row_top[:, None]), axis=-1))
            log_total = row_top + jnp.log(total_exp)
            hitting = columns[None, :] == block_label[:, None]
            label_logit = lax.optimization_barrier(jnp.sum(jnp.where(hitting, logits, 0.0), axis=-1))
            numerator = jnp.sum(block_weight * (log_total - label_logit))
            softmax = jnp.exp(logits - log_total[:, None])
            slopes = (factor * block_weight[:, None] * (softmax - hitting.astype(jnp.float32))).astype(jnp.bfloat16)
            update = jnp.dot(rows_wide.T, slopes.astype(jnp.float32), precision=lax.Precision.HIGHEST)
            return ((state_pair[0] + update, state_pair[1] + numerator), None)
        start_pair = (gradient, jnp.zeros((), jnp.float32))
        finished, ignored = lax.scan(one_block, start_pair, jnp.arange(TOKENS // block_rows, dtype=jnp.int32))
        gradient = finished[0]
        loss_total = loss_total + factor * finished[1] / counted
    return (loss_total, gradient)
```

```python
import functools

import jax
import jax.numpy as jnp
from jax import lax
from jax.experimental import pallas as pl
from jax.experimental.pallas import tpu as pltpu
from jax.sharding import PartitionSpec as P

WINDOW = 512
MAXOFF = 4

epsilon = 1e-05
step_decay = 0.8
MESH = pl.DeviceIdType.MESH


def spread_kernel(axes, sizes, *refs):
    count = len(axes)
    sources, targets = refs[:count], refs[count : 2 * count]
    held, sems = refs[2 * count : 3 * count], refs[3 * count :]
    barrier = pltpu.get_barrier_semaphore()
    peers = 0
    for axis, size in dict(zip(axes, sizes)).items():
        me = lax.axis_index(axis)
        for j in range(1, size):
            pl.semaphore_signal(
                barrier, inc=1, device_id={axis: lax.rem(me + j, size)}, device_id_type=MESH
            )
            peers += 1
    pl.semaphore_wait(barrier, peers)
    copies = []
    for k in range(count):
        me = lax.axis_index(axes[k])
        for j in range(1, sizes[k]):
            copy = pltpu.make_async_remote_copy(
                src_ref=sources[k],
                dst_ref=held[k].at[me],
                send_sem=sems[2 * k].at[j],
                recv_sem=sems[2 * k + 1].at[j],
                device_id={axes[k]: lax.rem(me + j, sizes[k])},
                device_id_type=MESH,
            )
            copy.start()
            copies.append(copy)
    for k in range(count):
        held[k][lax.axis_index(axes[k])] = sources[k][...]
    for copy in copies:
        copy.wait()
    for k in range(count):
        targets[k][...] = held[k][...]


def spread(pairs, identity):
    arrays = [a for a, _ in pairs]
    axes = [axis for _, axis in pairs]
    sizes = [lax.axis_size(axis) for axis in axes]
    shapes = [(size, *a.shape) for a, size in zip(arrays, sizes)]
    vmem = pl.BlockSpec(memory_space=pltpu.VMEM)
    sems = []
    for size in sizes:
        sems += [pltpu.SemaphoreType.DMA((size,))] * 2
    return pl.pallas_call(
        functools.partial(spread_kernel, axes, sizes),
        out_shape=[jax.ShapeDtypeStruct(s, a.dtype) for s, a in zip(shapes, arrays)],
        in_specs=[vmem] * len(arrays),
        out_specs=[vmem] * len(arrays),
        scratch_shapes=[pltpu.VMEM(s, a.dtype) for s, a in zip(shapes, arrays)] + sems,
        compiler_params=pltpu.CompilerParams(collective_id=identity, has_side_effects=True),
        name=f"spread{identity}",
    )(*arrays)


def logits_kernel(
    n, ways, normed, weight, gathered, logits, held, part, landed,
    send, recv, part_send, part_recv, out_sem, own_sem,
):
    steps, rows, vocab = part.shape[1:]
    mine = rows // ways
    line = n // 4
    me, rank = lax.axis_index("dp"), lax.axis_index("tensor")
    c, x, z = lax.rem(me, 2), lax.rem(me // 2, 2), me // 4
    sibling, other = 1 - c, 1 - x

    def at(z_, x_, c_):
        return (z_ * 2 + x_) * 2 + c_

    own = pltpu.make_async_copy(normed, held.at[me], own_sem)
    own.start()
    barrier = pltpu.get_barrier_semaphore()

    def greet(device):
        pl.semaphore_signal(barrier, inc=1, device_id=device, device_id_type=MESH)

    @pl.when(z > 0)
    def _():
        greet({"dp": at(z - 1, x, c)})

    @pl.when(z < line - 1)
    def _():
        greet({"dp": at(z + 1, x, c)})

    greet({"dp": at(z, other, c)})
    greet({"dp": at(z, x, sibling)})
    for j in range(1, ways):
        greet({"tensor": lax.rem(rank + j, ways)})
    chips = jnp.where(z > 0, 1, 0) + jnp.where(z < line - 1, 1, 0)
    pl.semaphore_wait(barrier, chips + 1 + ways)
    own.wait()

    def block_copy(kind, b, s, target):
        return pltpu.make_async_remote_copy(
            src_ref=held.at[b, s],
            dst_ref=held.at[b, s],
            send_sem=send.at[kind, b, s],
            recv_sem=recv.at[b, s],
            device_id={"dp": target},
            device_id_type=MESH,
        )

    def ups(b, s):
        return block_copy(0, b, s, at(z + 1, x, c))

    def downs(b, s):
        return block_copy(1, b, s, at(z - 1, x, c))

    def across(b, s):
        return block_copy(2, b, s, at(z, other, c))

    def beside(b, s):
        return block_copy(3, b, s, at(z, x, sibling))

    def part_copy(j, b, s):
        peer = lax.rem(rank + j, ways)
        return pltpu.make_async_remote_copy(
            src_ref=part.at[b, s, pl.ds(pl.multiple_of(peer * mine, mine), mine)],
            dst_ref=landed.at[j - 1, b, s],
            send_sem=part_send.at[j - 1, b, s],
            recv_sem=part_recv.at[j - 1, b, s],
            device_id={"tensor": peer},
            device_id_type=MESH,
        )

    def out_copy(b, s):
        return pltpu.make_async_copy(held.at[b, s], gathered.at[b, s], out_sem.at[b, s])

    def inside(zz):
        return jnp.logical_and(zz >= 0, zz < line)

    def stage(t, carry):
        k, s = t // steps, lax.rem(t, steps)
        for side in (0, 1):
            zz = z + k if side else z - k
            ok = jnp.logical_and(inside(zz), k > 0) if side else inside(zz)

            @pl.when(ok)
            def _(zz=zz):
                b = at(zz, x, c)

                @pl.when(k > 0)
                def _():
                    beside(b, s).wait_recv()

                @pl.when(jnp.logical_and(zz <= z, z < line - 1))
                def _():
                    ups(b, s).start()

                @pl.when(jnp.logical_and(zz >= z, z > 0))
                def _():
                    downs(b, s).start()

                across(b, s).start()
                beside(b, s).start()

        for side in (0, 1):
            zz = z + (k - 1) if side else z - (k - 1)
            ok = jnp.logical_and(inside(zz), k > side)

            @pl.when(ok)
            def _(zz=zz):
                b = at(zz, other, c)
                beside(b, s).wait_recv()
                beside(b, s).start()

        def multiply(q, carry):
            core, kind, side = q // 4, lax.rem(q // 2, 2), lax.rem(q, 2)
            away = k - kind
            zz = z + away * (2 * side - 1)
            ok = jnp.logical_and(inside(zz), away >= side)

            @pl.when(ok)
            def _():
                b = at(zz, lax.rem(x + kind, 2), lax.rem(c + core, 2))

                @pl.when(core > 0)
                def _():
                    beside(b, s).wait_recv()

                out_copy(b, s).start()
                part[b, s] = jnp.dot(held[b, s], weight[...], preferred_element_type=jnp.float32)
                for j in range(1, ways):
                    part_copy(j, b, s).start()

            return carry

        return lax.fori_loop(0, 8, multiply, carry)

    lax.fori_loop(0, (line + 1) * steps, stage, 0)

    def finish(u, carry):
        b, s = u // steps, lax.rem(u, steps)
        cb, xb, zb = lax.rem(b, 2), lax.rem(b // 2, 2), b // 4
        column = jnp.logical_and(xb == x, cb == c)

        @pl.when(jnp.logical_and(column, jnp.logical_and(zb <= z, z < line - 1)))
        def _():
            ups(b, s).wait_send()

        @pl.when(jnp.logical_and(column, jnp.logical_and(zb >= z, z > 0)))
        def _():
            downs(b, s).wait_send()

        @pl.when(column)
        def _():
            across(b, s).wait_send()

        @pl.when(cb == c)
        def _():
            beside(b, s).wait_send()

        out_copy(b, s).wait()
        for j in range(1, ways):
            part_copy(j, b, s).wait_recv()
        total = part[b, s, pl.ds(pl.multiple_of(rank * mine, mine), mine)]
        for j in range(1, ways):
            total += landed[j - 1, b, s]
        logits[b, s] = total
        for j in range(1, ways):
            part_copy(j, b, s).wait_send()
        return carry

    lax.fori_loop(0, n * steps, finish, 0)


def gather_and_multiply(normed, weight):
    steps, rows, width = normed.shape
    vocab = weight.shape[1]
    n, ways = lax.axis_size("dp"), lax.axis_size("tensor")
    mine = rows // ways
    vmem = pl.BlockSpec(memory_space=pltpu.VMEM)
    hbm = pl.BlockSpec(memory_space=pl.ANY)
    dma = pltpu.SemaphoreType.DMA
    return pl.pallas_call(
        functools.partial(logits_kernel, n, ways),
        out_shape=[
            jax.ShapeDtypeStruct((n, steps, rows, width), jnp.bfloat16),
            jax.ShapeDtypeStruct((n, steps, mine, vocab), jnp.float32),
        ],
        in_specs=[hbm, vmem],
        out_specs=[hbm, vmem],
        scratch_shapes=[
            pltpu.VMEM((n, steps, rows, width), jnp.bfloat16),
            pltpu.VMEM((n, steps, rows, vocab), jnp.float32),
            pltpu.VMEM((ways - 1, n, steps, mine, vocab), jnp.float32),
            dma((4, n, steps)),
            dma((n, steps)),
            dma((ways - 1, n, steps)),
            dma((ways - 1, n, steps)),
            dma((n, steps)),
            dma,
        ],
        compiler_params=pltpu.CompilerParams(
            collective_id=7, has_side_effects=True, vmem_limit_bytes=60 * 1024 * 1024
        ),
        name="gather_and_multiply",
    )(normed, weight)


def local(drafter_hidden, norm_gain, head_weight, labels, loss_mask, offsets):
    step_count, local_tokens, width_part = drafter_hidden.shape
    vocab_part = head_weight.shape[1]
    data_ways = lax.axis_size("dp")
    tensor_ways = lax.axis_size("tensor")
    data_rank = lax.axis_index("dp")
    tensor_rank = lax.axis_index("tensor")
    all_tokens = local_tokens * data_ways
    rows_each = local_tokens // tensor_ways
    hidden_wide = drafter_hidden.astype(jnp.float32)
    squares_all, token_all = spread(
        [
            (jnp.sum(hidden_wide * hidden_wide, axis=-1), "tensor"),
            (jnp.stack([labels, loss_mask]), "dp"),
        ],
        5,
    )
    inverse = lax.rsqrt(jnp.sum(squares_all, axis=0) / (width_part * tensor_ways) + epsilon)
    normed = (hidden_wide * inverse[:, :, None] * norm_gain.astype(jnp.float32)).astype(
        jnp.bfloat16
    )
    gathered, logits = gather_and_multiply(normed, head_weight)

    everywhere = jnp.arange(all_tokens, dtype=jnp.int32)

    def moved(values, by):
        padded = jnp.concatenate([values, jnp.broadcast_to(values[-1:], (MAXOFF,))])
        result = padded[MAXOFF : MAXOFF + all_tokens]
        for far in range(1, MAXOFF):
            result = jnp.where(by == far, padded[far : far + all_tokens], result)
        return result

    def own_rows(values):
        grid = values.reshape(data_ways, local_tokens)
        return lax.dynamic_slice_in_dim(grid, tensor_rank * rows_each, rows_each, 1)

    label_flat = token_all[:, 0].reshape(all_tokens)
    mask_flat = token_all[:, 1].reshape(all_tokens)
    label_list, weight_list, count_list = [], [], []
    for step_at in range(step_count):
        by = offsets[step_at]
        inside = everywhere % WINDOW + by < WINDOW
        weights = jnp.where(inside, moved(mask_flat, by), 0).astype(jnp.float32)
        count_list.append(jnp.sum(weights))
        weight_list.append(own_rows(weights))
        label_list.append(own_rows(moved(label_flat, by)))
    row_label = jnp.stack(label_list, axis=1)
    row_weight = jnp.stack(weight_list, axis=1)
    counted = jnp.stack(count_list)
    factors = step_decay ** jnp.arange(step_count, dtype=jnp.float32)

    columns = data_rank * vocab_part + jnp.arange(vocab_part, dtype=jnp.int32)
    hitting = columns == row_label[..., None]
    local_top = jnp.max(logits, axis=-1)
    label_part = jnp.sum(jnp.where(hitting, logits, 0.0), axis=-1)
    local_lse = local_top + jnp.log(jnp.sum(jnp.exp(logits - local_top[..., None]), axis=-1))
    (lse_all,) = spread([(local_lse.reshape(-1, local_tokens), "dp")], 6)
    top = jnp.max(lse_all, axis=0)
    log_total = (top + jnp.log(jnp.sum(jnp.exp(lse_all - top), axis=0))).reshape(local_lse.shape)
    softmax = jnp.exp(logits - log_total[..., None])
    slopes = (
        factors[:, None, None] * row_weight[..., None] * (softmax - hitting.astype(jnp.float32))
    ).astype(jnp.bfloat16)

    parts = [slopes]
    for far in range(1, tensor_ways):
        parts.append(
            lax.ppermute(
                slopes, "tensor", [(i, (i + far) % tensor_ways) for i in range(tensor_ways)]
            )
        )
    ordered = [
        lax.select_n(
            jnp.broadcast_to((tensor_rank - place) % tensor_ways == 1, slopes.shape), *parts
        )
        if tensor_ways == 2
        else lax.dynamic_index_in_dim(
            jnp.stack(parts), (tensor_rank - place) % tensor_ways, 0, False
        )
        for place in range(tensor_ways)
    ]
    gradient = jnp.einsum(
        "nsrd,nsrv->dv",
        gathered,
        jnp.concatenate(ordered, axis=2),
        preferred_element_type=jnp.float32,
    )

    shared = jnp.where(data_rank == 0, log_total, 0.0) - label_part
    numerator = lax.psum(jnp.sum(row_weight * shared, axis=(0, 2)), ("dp", "tensor"))
    loss_total = jnp.sum(factors * numerator / counted)
    return (loss_total, gradient)


def solution(mesh):
    return jax.shard_map(
        local,
        mesh=mesh,
        in_specs=(P(None, "dp", "tensor"), P("tensor"), P("tensor", "dp"), P("dp"), P("dp"), P()),
        out_specs=(P(), P("tensor", "dp")),
        check_vma=False,
    )
```

```python
import functools

import jax
import jax.numpy as jnp
from jax import lax
from jax.experimental import pallas as pl
from jax.experimental.pallas import tpu as pltpu
from jax.sharding import PartitionSpec as P

WINDOW = 512
MAXOFF = 4

epsilon = 1e-05
step_decay = 0.8
MESH = pl.DeviceIdType.MESH


def spread_kernel(axes, sizes, *refs):
    count = len(axes)
    sources, targets = refs[:count], refs[count : 2 * count]
    held, sems = refs[2 * count : 3 * count], refs[3 * count :]
    barrier = pltpu.get_barrier_semaphore()
    peers = 0
    for axis, size in dict(zip(axes, sizes)).items():
        me = lax.axis_index(axis)
        for j in range(1, size):
            pl.semaphore_signal(
                barrier, inc=1, device_id={axis: lax.rem(me + j, size)}, device_id_type=MESH
            )
            peers += 1
    pl.semaphore_wait(barrier, peers)
    copies = []
    for k in range(count):
        me = lax.axis_index(axes[k])
        for j in range(1, sizes[k]):
            copy = pltpu.make_async_remote_copy(
                src_ref=sources[k],
                dst_ref=held[k].at[me],
                send_sem=sems[2 * k].at[j],
                recv_sem=sems[2 * k + 1].at[j],
                device_id={axes[k]: lax.rem(me + j, sizes[k])},
                device_id_type=MESH,
            )
            copy.start()
            copies.append(copy)
    for k in range(count):
        held[k][lax.axis_index(axes[k])] = sources[k][...]
    for copy in copies:
        copy.wait()
    for k in range(count):
        targets[k][...] = held[k][...]


def spread(pairs, identity):
    arrays = [a for a, _ in pairs]
    axes = [axis for _, axis in pairs]
    sizes = [lax.axis_size(axis) for axis in axes]
    shapes = [(size, *a.shape) for a, size in zip(arrays, sizes)]
    vmem = pl.BlockSpec(memory_space=pltpu.VMEM)
    sems = []
    for size in sizes:
        sems += [pltpu.SemaphoreType.DMA((size,))] * 2
    return pl.pallas_call(
        functools.partial(spread_kernel, axes, sizes),
        out_shape=[jax.ShapeDtypeStruct(s, a.dtype) for s, a in zip(shapes, arrays)],
        in_specs=[vmem] * len(arrays),
        out_specs=[vmem] * len(arrays),
        scratch_shapes=[pltpu.VMEM(s, a.dtype) for s, a in zip(shapes, arrays)] + sems,
        compiler_params=pltpu.CompilerParams(collective_id=identity, has_side_effects=True),
        name=f"spread{identity}",
    )(*arrays)


def logits_kernel(
    n, ways, normed, weight, *refs
):
    gathered = refs[:ways]
    logits, held, part, landed, send, recv, part_send, part_recv, out_sem, own_sem = refs[ways:]
    steps, rows, vocab = part.shape[1:]
    mine = rows // ways
    line = n // 4
    me, rank = lax.axis_index("dp"), lax.axis_index("tensor")
    c, x, z = lax.rem(me, 2), lax.rem(me // 2, 2), me // 4
    sibling, other = 1 - c, 1 - x

    def at(z_, x_, c_):
        return (z_ * 2 + x_) * 2 + c_

    own = pltpu.make_async_copy(normed, held.at[me], own_sem)
    own.start()
    barrier = pltpu.get_barrier_semaphore()

    def greet(device):
        pl.semaphore_signal(barrier, inc=1, device_id=device, device_id_type=MESH)

    @pl.when(z > 0)
    def _():
        greet({"dp": at(z - 1, x, c)})

    @pl.when(z < line - 1)
    def _():
        greet({"dp": at(z + 1, x, c)})

    greet({"dp": at(z, other, c)})
    greet({"dp": at(z, x, sibling)})
    for j in range(1, ways):
        greet({"tensor": lax.rem(rank + j, ways)})
    chips = jnp.where(z > 0, 1, 0) + jnp.where(z < line - 1, 1, 0)
    pl.semaphore_wait(barrier, chips + 1 + ways)
    own.wait()

    def block_copy(kind, b, s, target):
        return pltpu.make_async_remote_copy(
            src_ref=held.at[b, s],
            dst_ref=held.at[b, s],
            send_sem=send.at[kind, b, s],
            recv_sem=recv.at[b, s],
            device_id={"dp": target},
            device_id_type=MESH,
        )

    def ups(b, s):
        return block_copy(0, b, s, at(z + 1, x, c))

    def downs(b, s):
        return block_copy(1, b, s, at(z - 1, x, c))

    def across(b, s):
        return block_copy(2, b, s, at(z, other, c))

    def beside(b, s):
        return block_copy(3, b, s, at(z, x, sibling))

    def part_copy(j, b, s):
        peer = lax.rem(rank + j, ways)
        return pltpu.make_async_remote_copy(
            src_ref=part.at[b, s, pl.ds(pl.multiple_of(peer * mine, mine), mine)],
            dst_ref=landed.at[j - 1, b, s],
            send_sem=part_send.at[j - 1, b, s],
            recv_sem=part_recv.at[j - 1, b, s],
            device_id={"tensor": peer},
            device_id_type=MESH,
        )

    def out_copy(far, b, s):
        owner = lax.rem(rank - far + ways, ways)
        return pltpu.make_async_copy(
            held.at[b, s, pl.ds(pl.multiple_of(owner * mine, mine), mine)],
            gathered[far].at[b, s],
            out_sem.at[far, b, s],
        )

    def inside(zz):
        return jnp.logical_and(zz >= 0, zz < line)

    def stage(t, carry):
        k, s = t // steps, lax.rem(t, steps)
        for side in (0, 1):
            zz = z + k if side else z - k
            ok = jnp.logical_and(inside(zz), k > 0) if side else inside(zz)

            @pl.when(ok)
            def _(zz=zz):
                b = at(zz, x, c)

                @pl.when(k > 0)
                def _():
                    beside(b, s).wait_recv()

                @pl.when(jnp.logical_and(zz <= z, z < line - 1))
                def _():
                    ups(b, s).start()

                @pl.when(jnp.logical_and(zz >= z, z > 0))
                def _():
                    downs(b, s).start()

                across(b, s).start()
                beside(b, s).start()

        for side in (0, 1):
            zz = z + (k - 1) if side else z - (k - 1)
            ok = jnp.logical_and(inside(zz), k > side)

            @pl.when(ok)
            def _(zz=zz):
                b = at(zz, other, c)
                beside(b, s).wait_recv()
                beside(b, s).start()

        def multiply(q, carry):
            core, kind, side = q // 4, lax.rem(q // 2, 2), lax.rem(q, 2)
            away = k - kind
            zz = z + away * (2 * side - 1)
            ok = jnp.logical_and(inside(zz), away >= side)

            @pl.when(ok)
            def _():
                b = at(zz, lax.rem(x + kind, 2), lax.rem(c + core, 2))

                @pl.when(core > 0)
                def _():
                    beside(b, s).wait_recv()

                for far in range(ways):
                    out_copy(far, b, s).start()
                part[b, s] = jnp.dot(held[b, s], weight[...], preferred_element_type=jnp.float32)
                for j in range(1, ways):
                    part_copy(j, b, s).start()

            return carry

        return lax.fori_loop(0, 8, multiply, carry)

    lax.fori_loop(0, (line + 1) * steps, stage, 0)

    def finish(u, carry):
        b, s = u // steps, lax.rem(u, steps)
        cb, xb, zb = lax.rem(b, 2), lax.rem(b // 2, 2), b // 4
        column = jnp.logical_and(xb == x, cb == c)

        @pl.when(jnp.logical_and(column, jnp.logical_and(zb <= z, z < line - 1)))
        def _():
            ups(b, s).wait_send()

        @pl.when(jnp.logical_and(column, jnp.logical_and(zb >= z, z > 0)))
        def _():
            downs(b, s).wait_send()

        @pl.when(column)
        def _():
            across(b, s).wait_send()

        @pl.when(cb == c)
        def _():
            beside(b, s).wait_send()

        for far in range(ways):
            out_copy(far, b, s).wait()
        for j in range(1, ways):
            part_copy(j, b, s).wait_recv()
        total = part[b, s, pl.ds(pl.multiple_of(rank * mine, mine), mine)]
        for j in range(1, ways):
            total += landed[j - 1, b, s]
        logits[b, s] = total
        for j in range(1, ways):
            part_copy(j, b, s).wait_send()
        return carry

    lax.fori_loop(0, n * steps, finish, 0)


def gather_and_multiply(normed, weight):
    steps, rows, width = normed.shape
    vocab = weight.shape[1]
    n, ways = lax.axis_size("dp"), lax.axis_size("tensor")
    mine = rows // ways
    vmem = pl.BlockSpec(memory_space=pltpu.VMEM)
    hbm = pl.BlockSpec(memory_space=pl.ANY)
    dma = pltpu.SemaphoreType.DMA
    return pl.pallas_call(
        functools.partial(logits_kernel, n, ways),
        out_shape=[
            *[jax.ShapeDtypeStruct((n, steps, mine, width), jnp.bfloat16)] * ways,
            jax.ShapeDtypeStruct((n, steps, mine, vocab), jnp.float32),
        ],
        in_specs=[hbm, vmem],
        out_specs=[hbm] * ways + [vmem],
        scratch_shapes=[
            pltpu.VMEM((n, steps, rows, width), jnp.bfloat16),
            pltpu.VMEM((n, steps, rows, vocab), jnp.float32),
            pltpu.VMEM((ways - 1, n, steps, mine, vocab), jnp.float32),
            dma((4, n, steps)),
            dma((n, steps)),
            dma((ways - 1, n, steps)),
            dma((ways - 1, n, steps)),
            dma((ways, n, steps)),
            dma,
        ],
        compiler_params=pltpu.CompilerParams(
            collective_id=7, has_side_effects=True, vmem_limit_bytes=60 * 1024 * 1024
        ),
        name="gather_and_multiply",
    )(normed, weight)


def local(drafter_hidden, norm_gain, head_weight, labels, loss_mask, offsets):
    step_count, local_tokens, width_part = drafter_hidden.shape
    vocab_part = head_weight.shape[1]
    data_ways = lax.axis_size("dp")
    tensor_ways = lax.axis_size("tensor")
    data_rank = lax.axis_index("dp")
    tensor_rank = lax.axis_index("tensor")
    all_tokens = local_tokens * data_ways
    rows_each = local_tokens // tensor_ways
    hidden_wide = drafter_hidden.astype(jnp.float32)
    squares_all, token_all = spread(
        [
            (jnp.sum(hidden_wide * hidden_wide, axis=-1), "tensor"),
            (jnp.stack([labels, loss_mask]), "dp"),
        ],
        5,
    )
    inverse = lax.rsqrt(jnp.sum(squares_all, axis=0) / (width_part * tensor_ways) + epsilon)
    normed = (hidden_wide * inverse[:, :, None] * norm_gain.astype(jnp.float32)).astype(
        jnp.bfloat16
    )
    *gathered, logits = gather_and_multiply(normed, head_weight)

    everywhere = jnp.arange(all_tokens, dtype=jnp.int32)

    def moved(values, by):
        padded = jnp.concatenate([values, jnp.broadcast_to(values[-1:], (MAXOFF,))])
        result = padded[MAXOFF : MAXOFF + all_tokens]
        for far in range(1, MAXOFF):
            result = jnp.where(by == far, padded[far : far + all_tokens], result)
        return result

    def own_rows(values):
        grid = values.reshape(data_ways, local_tokens)
        return lax.dynamic_slice_in_dim(grid, tensor_rank * rows_each, rows_each, 1)

    label_flat = token_all[:, 0].reshape(all_tokens)
    mask_flat = token_all[:, 1].reshape(all_tokens)
    label_list, weight_list, count_list = [], [], []
    for step_at in range(step_count):
        by = offsets[step_at]
        inside = everywhere % WINDOW + by < WINDOW
        weights = jnp.where(inside, moved(mask_flat, by), 0).astype(jnp.float32)
        count_list.append(jnp.sum(weights))
        weight_list.append(own_rows(weights))
        label_list.append(own_rows(moved(label_flat, by)))
    row_label = jnp.stack(label_list, axis=1)
    row_weight = jnp.stack(weight_list, axis=1)
    counted = jnp.stack(count_list)
    factors = step_decay ** jnp.arange(step_count, dtype=jnp.float32)

    columns = data_rank * vocab_part + jnp.arange(vocab_part, dtype=jnp.int32)
    hitting = columns == row_label[..., None]
    local_top = jnp.max(logits, axis=-1)
    label_part = jnp.sum(jnp.where(hitting, logits, 0.0), axis=-1)
    local_lse = local_top + jnp.log(jnp.sum(jnp.exp(logits - local_top[..., None]), axis=-1))
    label_sum = jnp.sum(row_weight * label_part, axis=(0, 2))
    lse_rows = local_lse.reshape(-1, local_tokens)
    label_rows = jnp.broadcast_to(label_sum[:, None], (step_count, local_tokens))
    (spread_all,) = spread([(jnp.concatenate([lse_rows, label_rows]), "dp")], 6)
    lse_all = spread_all[:, : lse_rows.shape[0]]
    label_total = jnp.sum(spread_all[:, lse_rows.shape[0] :, 0], axis=0)
    top = jnp.max(lse_all, axis=0)
    log_total = (top + jnp.log(jnp.sum(jnp.exp(lse_all - top), axis=0))).reshape(local_lse.shape)
    softmax = jnp.exp(logits - log_total[..., None])
    slopes = (
        factors[:, None, None] * row_weight[..., None] * (softmax - hitting.astype(jnp.float32))
    ).astype(jnp.bfloat16)

    parts = [slopes]
    for far in range(1, tensor_ways):
        parts.append(
            lax.ppermute(
                slopes, "tensor", [(i, (i + far) % tensor_ways) for i in range(tensor_ways)]
            )
        )
    gradient = sum(
        jnp.einsum("nsrd,nsrv->dv", rows, part, preferred_element_type=jnp.float32)
        for rows, part in zip(gathered, parts)
    )

    own_sum = jnp.sum(row_weight * log_total, axis=(0, 2)) - label_total
    (sums_all,) = spread(
        [(jnp.broadcast_to(own_sum[:, None], (step_count, local_tokens)), "tensor")], 8
    )
    numerator = jnp.sum(sums_all[:, :, 0], axis=0)
    loss_total = jnp.sum(factors * numerator / counted)
    return (loss_total, gradient)


def solution(mesh):
    return jax.shard_map(
        local,
        mesh=mesh,
        in_specs=(P(None, "dp", "tensor"), P("tensor"), P("tensor", "dp"), P("dp"), P("dp"), P()),
        out_specs=(P(), P("tensor", "dp")),
        check_vma=False,
    )
```
